32 devices in a mesh: dp: 8 (over z, y), pipe: 4 (over x, core).
Axes of the slice: x: 2, y: 2, z: 4, core: 2. Of those that a mesh axis runs over, the one named last changes fastest.
Arguments:
- inputs: bfloat16 [16, 64, 1024], P(None, 'dp'), may hold values from -6 to 6
- input_weight: bfloat16 [4, 1024, 4096], P('pipe'), may hold values from -0.1875 to 0.1875
- recurrent_weight: bfloat16 [4, 1024, 4096], P('pipe'), may hold values from -0.1875 to 0.1875
- gate_bias: float32 [4, 4096], P('pipe'), may hold values from -4 to 4
- lengths: int32 [64], P('dp'), may hold values from 1 to 16
- cotangent: bfloat16 [4, 16, 64, 1024], P('pipe', None, 'dp'), may hold values from -6 to 6
Outputs:
- grad_input: float32 [4, 1024, 4096], P('pipe', 'dp')
- grad_recurrent: float32 [4, 1024, 4096], P('pipe', 'dp')
- grad_bias: float32 [4, 4096], P('pipe', 'dp')
- final_hidden: bfloat16 [4, 64, 1024], P('pipe', 'dp')
- final_cell: float32 [4, 64, 1024], P('pipe', 'dp')
The draws below stay inside these ranges and needn't reach their ends.
All inputs are finite; a program needn't handle non-finite values.
Results may differ from the reference program's by a relative error of at most 0.004.
Values may be sent and summed in bfloat16 or wider, within the bound.
A program may use at most 128 MiB of HBM per device.

```python
from functools import partial
import jax
import jax.numpy as jnp
from jax import lax

H = 1024
G = 4096
FRAMES = 16
LAYERS = 4
BATCH = 64


def plant(values, stream_key, least, largest):
    spot = [jax.random.randint(jax.random.fold_in(stream_key, axis), (), 0, length) for axis, length in enumerate(values.shape)]
    longest = values.shape.index(max(values.shape))
    neighbour = spot[:longest] + [(spot[longest] + 1) % values.shape[longest]] + spot[longest + 1:]
    return values.at[tuple(spot)].set(least).at[tuple(neighbour)].set(largest)


def with_spikes(array, key, source, target, blocks, factor):
    owner, partner = [(jnp.arange(array.shape[dim]) // (array.shape[dim] // blocks)).reshape([-1 if axis == dim else 1 for axis in range(array.ndim)]) for dim in (source, target)]
    chosen = jax.random.permutation(key, blocks)[partner]
    strong = (owner == chosen) | (owner == (partner + blocks // 2) % blocks)
    return jnp.where(strong, factor * array, array)


def levels(own_key, extent, split, least, high):
    level, own = 1.0, jax.random.fold_in(own_key, 6)
    for dim, shards_of in split:
        heights = jnp.exp(jax.random.uniform(jax.random.fold_in(own, dim), (shards_of,), jnp.float32, least / len(split), high / len(split)))
        level = level * jnp.repeat(heights, extent[dim] // shards_of).reshape([-1 if axis == dim else 1 for axis in range(len(extent))])
    return level


def normal_values(rng, shape, width, reach, cuts=(), kind=jnp.bfloat16):
    loudness = levels(rng, shape, cuts, -0.22, 0.18) if cuts else 1.0
    drawn = jax.random.normal(rng, shape, jnp.float32) * width * loudness
    return jnp.minimum(jnp.maximum(drawn, -reach), reach).astype(kind)


def noise_with(rng, extent, scale, reach, pieces, heavy, kind=jnp.bfloat16):
    values = scale * jax.random.normal(rng, extent, jnp.float32)
    if pieces:
        values = values * levels(rng, extent, pieces, -0.22, 0.18)
    return jnp.clip(with_spikes(values, jax.random.fold_in(rng, 3), *heavy), -reach, reach).astype(kind)


def setup_inputs(seed: int = 0) -> dict:
    keys = jax.random.split(jax.random.key(seed), 7)
    inputs = noise_with(keys[0], (FRAMES, BATCH, H), 1.0, 6.0, ((1, 8),), (1, 2, 8, 2.0))
    input_weight = normal_values(keys[1], (LAYERS, H, G), H ** -0.5, 0.1875, ((0, 4),))
    recurrent_weight = normal_values(keys[2], (LAYERS, H, G), H ** -0.5, 0.1875, ((0, 4),))
    gate_bias = normal_values(keys[3], (LAYERS, G), 1.0, 4.0, ((0, 4),), jnp.float32)
    lengths = plant(jax.random.randint(keys[4], (BATCH,), 1, FRAMES + 1), jax.random.fold_in(keys[4], 1), 1, FRAMES).astype(jnp.int32)
    cotangent = normal_values(keys[5], (LAYERS, FRAMES, BATCH, H), 1.0, 6.0, ((0, 4), (2, 8)))
    return {"inputs": inputs, "input_weight": input_weight, "recurrent_weight": recurrent_weight, "gate_bias": gate_bias, "lengths": lengths, "cotangent": cotangent}


def squash(value):
    return 1.0 / (1.0 + jnp.exp(-value))


def activate(pre_act, hidden_width):
    return jnp.concatenate([squash(pre_act[:, :2 * hidden_width]), jnp.tanh(pre_act[:, 2 * hidden_width:3 * hidden_width]), squash(pre_act[:, 3 * hidden_width:])], axis=1)


def forward_step(recurrent_weight, gate_bias, carry_state, step_inputs):
    hidden, cell_state = carry_state
    projected, alive_mask = step_inputs
    hidden_width = hidden.shape[1]
    pre_act = projected + jnp.dot(hidden, recurrent_weight, preferred_element_type=jnp.float32) + gate_bias
    gate_values = activate(pre_act, hidden_width)
    input_gate = gate_values[:, :hidden_width]
    forget_gate = gate_values[:, hidden_width:2 * hidden_width]
    cell_gate = gate_values[:, 2 * hidden_width:3 * hidden_width]
    output_gate = gate_values[:, 3 * hidden_width:]
    new_cell = forget_gate * cell_state + input_gate * cell_gate
    cand_hidden = (output_gate * jnp.tanh(new_cell)).astype(jnp.bfloat16)
    kept_cell = alive_mask * new_cell + (1.0 - alive_mask) * cell_state
    kept_hidden = jnp.where(alive_mask > 0, cand_hidden, hidden)
    emitted = jnp.where(alive_mask > 0, cand_hidden, jnp.zeros_like(cand_hidden))
    return (kept_hidden, kept_cell), (emitted, gate_values, kept_cell, hidden, cell_state)


def backward_step(recurrent_weight, carry_state, step_inputs):
    hidden_grad, cell_grad = carry_state
    upper_grad, own_grad, gate_values, cell_now, cell_prev, alive_mask = step_inputs
    hidden_width = hidden_grad.shape[1]
    input_gate = gate_values[:, :hidden_width]
    forget_gate = gate_values[:, hidden_width:2 * hidden_width]
    cell_gate = gate_values[:, 2 * hidden_width:3 * hidden_width]
    output_gate = gate_values[:, 3 * hidden_width:]
    out_grad = alive_mask * (hidden_grad + upper_grad.astype(jnp.float32) + own_grad.astype(jnp.float32))
    cell_tanh = jnp.tanh(cell_now)
    through_cell = alive_mask * cell_grad + out_grad * output_gate * (1.0 - cell_tanh * cell_tanh)
    pre_grad = jnp.concatenate([through_cell * cell_gate * input_gate * (1.0 - input_gate), through_cell * cell_prev * forget_gate * (1.0 - forget_gate), through_cell * input_gate * (1.0 - cell_gate * cell_gate), out_grad * cell_tanh * output_gate * (1.0 - output_gate)], axis=1).astype(jnp.bfloat16)
    back_hidden = (1.0 - alive_mask) * hidden_grad + lax.dot_general(pre_grad, recurrent_weight, (((1,), (1,)), ((), ())), preferred_element_type=jnp.float32)
    back_cell = (1.0 - alive_mask) * cell_grad + through_cell * forget_gate
    return (back_hidden, back_cell), pre_grad


def contract_rows(left, right):
    return lax.dot_general(left, right, (((0,), (0,)), ((), ())), preferred_element_type=jnp.float32)


def reference(inputs, input_weight, recurrent_weight, gate_bias, lengths, cotangent):
    frame_total, utterances, hidden_width = inputs.shape
    gate_width = 4 * hidden_width
    alive_all = (jnp.arange(frame_total, dtype=jnp.int32)[:, None] < lengths[None, :]).astype(jnp.float32)[:, :, None]
    layer_in = inputs
    saved = []
    last_hidden = []
    last_cell = []
    for layer_number in range(LAYERS):
        projected = jnp.dot(layer_in.reshape(-1, hidden_width), input_weight[layer_number], preferred_element_type=jnp.float32).reshape(frame_total, utterances, gate_width)
        start_state = (jnp.zeros((utterances, hidden_width), jnp.bfloat16), jnp.zeros((utterances, hidden_width), jnp.float32))
        (hidden, cell_state), records = lax.scan(partial(forward_step, recurrent_weight[layer_number], gate_bias[layer_number]), start_state, (projected, alive_all))
        emitted, gate_values, kept_cells, hidden_prev, cell_prev = records
        saved.append((layer_in, gate_values, kept_cells, hidden_prev, cell_prev))
        last_hidden.append(hidden)
        last_cell.append(cell_state)
        layer_in = emitted
    upper_grad = jnp.zeros((frame_total, utterances, hidden_width), jnp.bfloat16)
    grads_in = []
    grads_rec = []
    grads_bias = []
    for layer_number in reversed(range(LAYERS)):
        layer_in, gate_values, kept_cells, hidden_prev, cell_prev = saved[layer_number]
        zero_state = (jnp.zeros((utterances, hidden_width), jnp.float32), jnp.zeros((utterances, hidden_width), jnp.float32))
        final_carry, pre_grad = lax.scan(partial(backward_step, recurrent_weight[layer_number]), zero_state, (upper_grad, cotangent[layer_number], gate_values, kept_cells, cell_prev, alive_all), reverse=True)
        flat_grad = pre_grad.reshape(-1, gate_width)
        grads_in.append(contract_rows(layer_in.reshape(-1, hidden_width), flat_grad))
        grads_rec.append(contract_rows(hidden_prev.reshape(-1, hidden_width), flat_grad))
        grads_bias.append(jnp.sum(flat_grad.astype(jnp.float32), axis=0))
        upper_grad = lax.dot_general(flat_grad, input_weight[layer_number], (((1,), (1,)), ((), ())), preferred_element_type=jnp.float32).astype(jnp.bfloat16).reshape(frame_total, utterances, hidden_width)
    grad_input = jnp.stack(grads_in[::-1])
    grad_recurrent = jnp.stack(grads_rec[::-1])
    grad_bias = jnp.stack(grads_bias[::-1])
    return (grad_input, grad_recurrent, grad_bias, jnp.stack(last_hidden), jnp.stack(last_cell))
```

```python
from functools import partial

import jax
import jax.numpy as jnp
from jax import lax
from jax.experimental import pallas as pl
from jax.experimental.pallas import tpu as pltpu
from jax.sharding import PartitionSpec as P

SPAN = 2
MESH = pl.DeviceIdType.MESH
F32 = jnp.float32
BF16 = jnp.bfloat16


def squash(value):
    return 1.0 / (1.0 + jnp.exp(-value))


def rows_of(ref, start):
    pieces = [ref[start + b].astype(F32) for b in range(SPAN)]
    return jnp.concatenate(pieces, axis=0).astype(BF16)


def kernel(
    dp_total, pipe_total, own_width, share,
    inputs, input_weight, recurrent_weight, bias, alive, cotangent,
    dpre_all, x_all, h_all, final_hidden, final_cell,
    w, r, xin, y, hist, cells, gates, proj, dpre, upper, lower, dh, dc,
    load_sem, fsend, frecv, bsend, brecv, dsend, drecv, xsend, xrecv, hsend, hrecv, local_sem,
):
    frames, utterances, width = xin.shape
    blocks = frames // SPAN
    me = lax.axis_index("dp")
    stage = lax.axis_index("pipe")
    first = stage == 0
    last = stage == pipe_total - 1

    load_w = pltpu.make_async_copy(input_weight, w, load_sem.at[0])
    load_r = pltpu.make_async_copy(recurrent_weight, r, load_sem.at[1])
    load_x = pltpu.make_async_copy(inputs, xin, load_sem.at[2])

    @pl.when(first)
    def _():
        load_x.start()

    load_w.start()
    load_r.start()

    barrier = pltpu.get_barrier_semaphore()

    def greet(j, carry):
        peer = lax.rem(me + j, dp_total)
        pl.semaphore_signal(barrier, inc=1, device_id=(peer, stage), device_id_type=MESH)
        return carry

    lax.fori_loop(1, dp_total, greet, 0)

    for near in (1, pipe_total - 1):
        neighbour = lax.rem(stage + near, pipe_total)
        pl.semaphore_signal(barrier, inc=1, device_id=(me, neighbour), device_id_type=MESH)
    pl.semaphore_wait(barrier, dp_total + 1)

    def up(k):
        part = pl.ds(k * SPAN, SPAN)
        return pltpu.make_async_remote_copy(
            src_ref=y.at[part], dst_ref=xin.at[part], send_sem=fsend.at[k], recv_sem=frecv.at[k],
            device_id=(me, lax.rem(stage + 1, pipe_total)), device_id_type=MESH,
        )

    def down(k):
        part = pl.ds(k * SPAN, SPAN)
        return pltpu.make_async_remote_copy(
            src_ref=lower.at[part], dst_ref=upper.at[part], send_sem=bsend.at[k], recv_sem=brecv.at[k],
            device_id=(me, lax.rem(stage + pipe_total - 1, pipe_total)), device_id_type=MESH,
        )

    def spread(j, part, slot):
        peer = lax.rem(me + j, dp_total)
        return pltpu.make_async_remote_copy(
            src_ref=dpre.at[part], dst_ref=dpre_all.at[slot, part],
            send_sem=dsend.at[j - 1], recv_sem=drecv.at[j - 1],
            device_id=(peer, stage), device_id_type=MESH,
        )

    def columns(peer):
        return pl.ds(pl.multiple_of(((peer * own_width) // share) * share, 128), share)

    def hand_x(j, slot):
        peer = lax.rem(me + j, dp_total)
        return pltpu.make_async_remote_copy(
            src_ref=xin.at[:, :, columns(peer)], dst_ref=x_all.at[slot],
            send_sem=xsend.at[j - 1], recv_sem=xrecv.at[j - 1],
            device_id=(peer, stage), device_id_type=MESH,
        )

    def hand_h(j, slot):
        peer = lax.rem(me + j, dp_total)
        return pltpu.make_async_remote_copy(
            src_ref=hist.at[pl.ds(0, frames), :, columns(peer)], dst_ref=h_all.at[slot],
            send_sem=hsend.at[j - 1], recv_sem=hrecv.at[j - 1],
            device_id=(peer, stage), device_id_type=MESH,
        )

    own_x = pltpu.make_async_copy(xin.at[:, :, columns(me)], x_all.at[me], local_sem.at[0])
    own_h = pltpu.make_async_copy(
        hist.at[pl.ds(0, frames), :, columns(me)], h_all.at[me], local_sem.at[1]
    )
    own_d = pltpu.make_async_copy(dpre, dpre_all.at[me], local_sem.at[2])

    hist[0] = jnp.zeros((utterances, width), BF16)
    cells[0] = jnp.zeros((utterances, width), F32)

    @pl.when(first)
    def _():
        load_x.wait()

    load_w.wait()
    load_r.wait()

    def forward_block(k, carry):
        start = k * SPAN

        @pl.when(stage > 0)
        def _():
            up(k).wait_recv()

        got = jnp.dot(rows_of(xin, start), w[...], preferred_element_type=F32)
        for b in range(SPAN):
            proj[b] = got[b * utterances : (b + 1) * utterances]

        def step(b, inner):
            t = start + b
            hidden = hist[t]
            cell = cells[t]
            live = alive[t][:, :1]
            pre = proj[b] + jnp.dot(hidden, r[...], preferred_element_type=F32) + bias[...]
            i = squash(pre[:, :width])
            f = squash(pre[:, width : 2 * width])
            g = jnp.tanh(pre[:, 2 * width : 3 * width])
            o = squash(pre[:, 3 * width :])
            gates[t, :, pl.ds(0, width)] = i
            gates[t, :, pl.ds(width, width)] = f
            gates[t, :, pl.ds(2 * width, width)] = g
            gates[t, :, pl.ds(3 * width, width)] = o
            new_cell = f * cell + i * g
            cand = o * jnp.tanh(new_cell)
            cells[t + 1] = live * new_cell + (1.0 - live) * cell
            hist[t + 1] = jnp.where(live > 0, cand, hidden.astype(F32)).astype(BF16)
            y[t] = jnp.where(live > 0, cand, 0.0).astype(BF16)
            return inner

        lax.fori_loop(0, SPAN, step, 0)

        @pl.when(stage < pipe_total - 1)
        def _():
            up(k).start()

        return carry

    lax.fori_loop(0, blocks, forward_block, 0)
    final_hidden[...] = hist[frames]
    final_cell[...] = cells[frames]

    def hand(j, carry):
        hand_x(j, me).start()
        hand_h(j, me).start()
        return carry

    lax.fori_loop(1, dp_total, hand, 0)
    own_x.start()
    own_h.start()

    dh[...] = jnp.zeros(dh.shape, F32)
    dc[...] = jnp.zeros(dc.shape, F32)

    @pl.when(last)
    def _():
        upper[...] = jnp.zeros(upper.shape, BF16)

    nt = (((1,), (1,)), ((), ()))

    def backward_block(n, carry):
        k = blocks - 1 - n
        start = k * SPAN

        @pl.when(stage < pipe_total - 1)
        def _():
            down(k).wait_recv()

        def step(m, inner):
            t = start + SPAN - 1 - m
            live = alive[t][:, :1]
            i = gates[t, :, pl.ds(0, width)]
            f = gates[t, :, pl.ds(width, width)]
            g = gates[t, :, pl.ds(2 * width, width)]
            o = gates[t, :, pl.ds(3 * width, width)]
            e = live * (dh[...] + upper[t].astype(F32) + cotangent[t].astype(F32))
            tanh_c = jnp.tanh(cells[t + 1])
            dcell = live * dc[...] + e * o * (1.0 - tanh_c * tanh_c)
            dpre[t, :, pl.ds(0, width)] = (dcell * g * i * (1.0 - i)).astype(BF16)
            dpre[t, :, pl.ds(width, width)] = (dcell * cells[t] * f * (1.0 - f)).astype(BF16)
            dpre[t, :, pl.ds(2 * width, width)] = (dcell * i * (1.0 - g * g)).astype(BF16)
            dpre[t, :, pl.ds(3 * width, width)] = (e * tanh_c * o * (1.0 - o)).astype(BF16)
            back = lax.dot_general(dpre[t], r[...], nt, preferred_element_type=F32)
            dh[...] = (1.0 - live) * dh[...] + back
            dc[...] = (1.0 - live) * dc[...] + dcell * f
            return inner

        lax.fori_loop(0, SPAN, step, 0)

        @pl.when(stage > 0)
        def _():
            got = lax.dot_general(rows_of(dpre, start), w[...], nt, preferred_element_type=F32)
            for b in range(SPAN):
                lower[start + b] = got[b * utterances : (b + 1) * utterances].astype(BF16)
            down(k).start()

        def send(j, inner):
            spread(j, pl.ds(start, SPAN), me).start()
            return inner

        lax.fori_loop(1, dp_total, send, 0)
        return carry

    lax.fori_loop(0, blocks, backward_block, 0)
    own_d.start()

    def settle(j, carry):
        source = lax.rem(me + dp_total - j, dp_total)
        for copy in (hand_x(j, source), hand_h(j, source), spread(j, pl.ds(0, frames), source)):
            copy.wait_send()
            copy.wait_recv()
        return carry

    lax.fori_loop(1, dp_total, settle, 0)

    def drain(k, carry):
        @pl.when(stage < pipe_total - 1)
        def _():
            up(k).wait_send()

        @pl.when(stage > 0)
        def _():
            down(k).wait_send()

        return carry

    lax.fori_loop(0, blocks, drain, 0)
    own_x.wait()
    own_h.wait()
    own_d.wait()


def contract_rows(left, right):
    return lax.dot_general(
        left, right, (((0,), (0,)), ((), ())), preferred_element_type=F32
    )


def local(inputs, input_weight, recurrent_weight, gate_bias, lengths, cotangent):
    frames, utterances, width = inputs.shape
    gate_width = 4 * width
    dp_total = lax.axis_size("dp")
    pipe_total = lax.axis_size("pipe")
    me = lax.axis_index("dp")
    own_width = width // dp_total
    share = max(own_width, 128)
    blocks = frames // SPAN
    live = (jnp.arange(frames, dtype=jnp.int32)[:, None] < lengths[None, :]).astype(F32)
    live = jnp.broadcast_to(live[:, :, None], (frames, utterances, 128))
    vmem = pl.BlockSpec(memory_space=pltpu.VMEM)
    hbm = pl.BlockSpec(memory_space=pl.ANY)
    dma = pltpu.SemaphoreType.DMA
    dpre_all, x_all, h_all, hidden, cell = pl.pallas_call(
        partial(kernel, dp_total, pipe_total, own_width, share),
        out_shape=(
            jax.ShapeDtypeStruct((dp_total, frames, utterances, gate_width), BF16),
            jax.ShapeDtypeStruct((dp_total, frames, utterances, share), BF16),
            jax.ShapeDtypeStruct((dp_total, frames, utterances, share), BF16),
            jax.ShapeDtypeStruct((utterances, width), BF16),
            jax.ShapeDtypeStruct((utterances, width), F32),
        ),
        in_specs=[hbm, hbm, hbm, vmem, vmem, vmem],
        out_specs=(hbm, hbm, hbm, vmem, vmem),
        scratch_shapes=[
            pltpu.VMEM((width, gate_width), BF16),
            pltpu.VMEM((width, gate_width), BF16),
            pltpu.VMEM((frames, utterances, width), BF16),
            pltpu.VMEM((frames, utterances, width), BF16),
            pltpu.VMEM((frames + 1, utterances, width), BF16),
            pltpu.VMEM((frames + 1, utterances, width), F32),
            pltpu.VMEM((frames, utterances, gate_width), F32),
            pltpu.VMEM((SPAN, utterances, gate_width), F32),
            pltpu.VMEM((frames, utterances, gate_width), BF16),
            pltpu.VMEM((frames, utterances, width), BF16),
            pltpu.VMEM((frames, utterances, width), BF16),
            pltpu.VMEM((utterances, width), F32),
            pltpu.VMEM((utterances, width), F32),
            dma((3,)),
            dma((blocks,)),
            dma((blocks,)),
            dma((blocks,)),
            dma((blocks,)),
            dma((dp_total - 1,)),
            dma((dp_total - 1,)),
            dma((dp_total - 1,)),
            dma((dp_total - 1,)),
            dma((dp_total - 1,)),
            dma((dp_total - 1,)),
            dma((3,)),
        ],
        compiler_params=pltpu.CompilerParams(
            collective_id=0, has_side_effects=True, vmem_limit_bytes=48 * 1024 * 1024
        ),
    )(inputs, input_weight[0], recurrent_weight[0], gate_bias, live, cotangent[0])
    if share > own_width:
        offset = (me * own_width) % share
        x_all = lax.dynamic_slice_in_dim(x_all, offset, own_width, 3)
        h_all = lax.dynamic_slice_in_dim(h_all, offset, own_width, 3)
    rows = dpre_all.reshape(-1, gate_width)
    input_grad = contract_rows(x_all.reshape(-1, own_width), rows)
    recurrent_grad = contract_rows(h_all.reshape(-1, own_width), rows)
    bias_width = gate_width // dp_total
    mine = lax.dynamic_slice_in_dim(rows, me * bias_width, bias_width, 1)
    bias_grad = jnp.sum(mine.astype(F32), axis=0)
    return (input_grad[None], recurrent_grad[None], bias_grad[None], hidden[None], cell[None])


def solution(mesh):
    return jax.shard_map(
        local,
        mesh=mesh,
        in_specs=(
            P(None, "dp", None),
            P("pipe", None, None),
            P("pipe", None, None),
            P("pipe", None),
            P("dp"),
            P("pipe", None, "dp", None),
        ),
        out_specs=(
            P("pipe", "dp", None),
            P("pipe", "dp", None),
            P("pipe", "dp"),
            P("pipe", "dp", None),
            P("pipe", "dp", None),
        ),
        check_vma=False,
    )
```

```python
from functools import partial

import jax
import jax.numpy as jnp
from jax import lax
from jax.experimental import pallas as pl
from jax.experimental.pallas import tpu as pltpu
from jax.sharding import PartitionSpec as P

SPAN = 2
MESH = pl.DeviceIdType.MESH
F32 = jnp.float32
BF16 = jnp.bfloat16


def squash(value):
    return 1.0 / (1.0 + jnp.exp(-value))


def rows_of(ref, start):
    pieces = [ref[start + b].astype(F32) for b in range(SPAN)]
    return jnp.concatenate(pieces, axis=0).astype(BF16)


def kernel(
    dp_total, pipe_total, own_width, share,
    inputs, input_weight, recurrent_weight, bias, alive, cotangent,
    dpre_all, x_all, h_all, final_hidden, final_cell,
    w, r, w_turned, r_turned, xin, y, hist, cells, gates, proj, dpre, upper, lower, dh, dc,
    load_sem, fsend, frecv, bsend, brecv, psend, precv, dsend, drecv, wsend, wrecv, xsend, xrecv, hsend, hrecv, local_sem,
):
    frames, utterances, width = xin.shape
    blocks = frames // SPAN
    me = lax.axis_index("dp")
    stage = lax.axis_index("pipe")
    first = stage == 0
    last = stage == pipe_total - 1

    load_w = pltpu.make_async_copy(input_weight, w, load_sem.at[0])
    load_r = pltpu.make_async_copy(recurrent_weight, r, load_sem.at[1])
    load_x = pltpu.make_async_copy(inputs, xin, load_sem.at[2])

    @pl.when(first)
    def _():
        load_x.start()

    load_w.start()
    load_r.start()

    barrier = pltpu.get_barrier_semaphore()

    def greet(j, carry):
        peer = lax.rem(me + j, dp_total)
        pl.semaphore_signal(barrier, inc=1, device_id=(peer, stage), device_id_type=MESH)
        return carry

    lax.fori_loop(1, dp_total, greet, 0)

    for near in (1, pipe_total - 1):
        neighbour = lax.rem(stage + near, pipe_total)
        pl.semaphore_signal(barrier, inc=1, device_id=(me, neighbour), device_id_type=MESH)
    pl.semaphore_wait(barrier, dp_total + 1)

    def up(k):
        part = pl.ds(k * SPAN, SPAN)
        return pltpu.make_async_remote_copy(
            src_ref=y.at[part], dst_ref=xin.at[part], send_sem=fsend.at[k], recv_sem=frecv.at[k],
            device_id=(me, lax.rem(stage + 1, pipe_total)), device_id_type=MESH,
        )

    def down(k):
        part = pl.ds(k * SPAN, SPAN)
        return pltpu.make_async_remote_copy(
            src_ref=lower.at[part], dst_ref=upper.at[part], send_sem=bsend.at[k], recv_sem=brecv.at[k],
            device_id=(me, lax.rem(stage + pipe_total - 1, pipe_total)), device_id_type=MESH,
        )

    partner = me + 1 - 2 * lax.rem(me, 2)

    def to_partner(part, slot):
        return pltpu.make_async_remote_copy(
            src_ref=dpre.at[part], dst_ref=dpre_all.at[slot, part],
            send_sem=psend.at[0], recv_sem=precv.at[0],
            device_id=(partner, stage), device_id_type=MESH,
        )

    def spread(j, k, part, slot):
        peer = lax.rem(me + 2 * j, dp_total)
        return pltpu.make_async_remote_copy(
            src_ref=dpre.at[part], dst_ref=dpre_all.at[slot, part],
            send_sem=dsend.at[j - 1], recv_sem=drecv.at[(j - 1) * blocks + k],
            device_id=(peer, stage), device_id_type=MESH,
        )

    def relay(j, part, slot):
        return pltpu.make_async_remote_copy(
            src_ref=dpre_all.at[slot, part], dst_ref=dpre_all.at[slot, part],
            send_sem=wsend.at[j - 1], recv_sem=wrecv.at[j - 1],
            device_id=(partner, stage), device_id_type=MESH,
        )

    def source_of(device, j):
        return lax.rem(device + dp_total - 2 * j, dp_total)

    def relay_block(k):
        part = pl.ds(k * SPAN, SPAN)

        def one(j, inner):
            source = source_of(me, j)
            spread(j, k, part, source).wait_recv()
            relay(j, part, source).start()
            return inner

        lax.fori_loop(1, dp_total // 2, one, 0)

    tile = 256

    def turn(c, carry):
        cut = pl.ds(pl.multiple_of(c * tile, tile), tile)
        r_turned[cut, :] = r[:, cut].T
        w_turned[cut, :] = w[:, cut].T
        return carry

    turns = w.shape[1] // tile

    def columns(peer):
        return pl.ds(pl.multiple_of(((peer * own_width) // share) * share, 128), share)

    def hand_x(j, slot):
        peer = lax.rem(me + j, dp_total)
        return pltpu.make_async_remote_copy(
            src_ref=xin.at[:, :, columns(peer)], dst_ref=x_all.at[slot],
            send_sem=xsend.at[j - 1], recv_sem=xrecv.at[j - 1],
            device_id=(peer, stage), device_id_type=MESH,
        )

    def hand_h(j, slot):
        peer = lax.rem(me + j, dp_total)
        return pltpu.make_async_remote_copy(
            src_ref=hist.at[pl.ds(0, frames), :, columns(peer)], dst_ref=h_all.at[slot],
            send_sem=hsend.at[j - 1], recv_sem=hrecv.at[j - 1],
            device_id=(peer, stage), device_id_type=MESH,
        )

    own_x = pltpu.make_async_copy(xin.at[:, :, columns(me)], x_all.at[me], local_sem.at[0])
    own_h = pltpu.make_async_copy(
        hist.at[pl.ds(0, frames), :, columns(me)], h_all.at[me], local_sem.at[1]
    )
    own_d = pltpu.make_async_copy(dpre, dpre_all.at[me], local_sem.at[2])

    hist[0] = jnp.zeros((utterances, width), BF16)
    cells[0] = jnp.zeros((utterances, width), F32)

    @pl.when(first)
    def _():
        load_x.wait()

    load_w.wait()

    @pl.when(stage >= pipe_total // 2)
    def _():
        load_r.wait()
        lax.fori_loop(0, turns, turn, 0)


    def forward_block(k, carry):
        start = k * SPAN

        @pl.when(stage > 0)
        def _():
            up(k).wait_recv()

        got = jnp.dot(rows_of(xin, start), w[...], preferred_element_type=F32)
        for b in range(SPAN):
            proj[b] = got[b * utterances : (b + 1) * utterances]

        @pl.when((k == 0) & (stage < pipe_total // 2))
        def _():
            load_r.wait()

        def step(b, inner):
            t = start + b
            hidden = hist[t]
            cell = cells[t]
            live = alive[t][:, :1]
            pre = proj[b] + jnp.dot(hidden, r[...], preferred_element_type=F32) + bias[...]
            i = squash(pre[:, :width])
            f = squash(pre[:, width : 2 * width])
            g = jnp.tanh(pre[:, 2 * width : 3 * width])
            o = squash(pre[:, 3 * width :])
            gates[t, :, pl.ds(0, width)] = i
            gates[t, :, pl.ds(width, width)] = f
            gates[t, :, pl.ds(2 * width, width)] = g
            gates[t, :, pl.ds(3 * width, width)] = o
            new_cell = f * cell + i * g
            cand = o * jnp.tanh(new_cell)
            cells[t + 1] = live * new_cell + (1.0 - live) * cell
            hist[t + 1] = jnp.where(live > 0, cand, hidden.astype(F32)).astype(BF16)
            y[t] = jnp.where(live > 0, cand, 0.0).astype(BF16)
            return inner

        lax.fori_loop(0, SPAN, step, 0)

        @pl.when(stage < pipe_total - 1)
        def _():
            up(k).start()

        return carry

    lax.fori_loop(0, blocks, forward_block, 0)
    final_hidden[...] = hist[frames]
    final_cell[...] = cells[frames]

    def hand(j, carry):
        hand_x(j, me).start()
        hand_h(j, me).start()
        return carry

    lax.fori_loop(1, dp_total, hand, 0)
    own_x.start()
    own_h.start()

    @pl.when(stage < pipe_total // 2)
    def _():
        lax.fori_loop(0, turns, turn, 0)

    dh[...] = jnp.zeros(dh.shape, F32)
    dc[...] = jnp.zeros(dc.shape, F32)

    @pl.when(last)
    def _():
        upper[...] = jnp.zeros(upper.shape, BF16)

    def backward_block(n, carry):
        k = blocks - 1 - n
        start = k * SPAN

        @pl.when(stage < pipe_total - 1)
        def _():
            down(k).wait_recv()

        def step(m, inner):
            t = start + SPAN - 1 - m
            live = alive[t][:, :1]
            i = gates[t, :, pl.ds(0, width)]
            f = gates[t, :, pl.ds(width, width)]
            g = gates[t, :, pl.ds(2 * width, width)]
            o = gates[t, :, pl.ds(3 * width, width)]
            e = live * (dh[...] + upper[t].astype(F32) + cotangent[t].astype(F32))
            tanh_c = jnp.tanh(cells[t + 1])
            dcell = live * dc[...] + e * o * (1.0 - tanh_c * tanh_c)
            dpre[t, :, pl.ds(0, width)] = (dcell * g * i * (1.0 - i)).astype(BF16)
            dpre[t, :, pl.ds(width, width)] = (dcell * cells[t] * f * (1.0 - f)).astype(BF16)
            dpre[t, :, pl.ds(2 * width, width)] = (dcell * i * (1.0 - g * g)).astype(BF16)
            dpre[t, :, pl.ds(3 * width, width)] = (e * tanh_c * o * (1.0 - o)).astype(BF16)
            back = jnp.dot(dpre[t], r_turned[...], preferred_element_type=F32)
            dh[...] = (1.0 - live) * dh[...] + back
            dc[...] = (1.0 - live) * dc[...] + dcell * f
            return inner

        lax.fori_loop(0, SPAN, step, 0)

        @pl.when(stage > 0)
        def _():
            got = jnp.dot(rows_of(dpre, start), w_turned[...], preferred_element_type=F32)
            for b in range(SPAN):
                lower[start + b] = got[b * utterances : (b + 1) * utterances].astype(BF16)
            down(k).start()

        def send(j, inner):
            spread(j, k, pl.ds(start, SPAN), me).start()
            return inner

        lax.fori_loop(1, dp_total // 2, send, 0)
        to_partner(pl.ds(start, SPAN), me).start()

        @pl.when(n > 0)
        def _():
            relay_block(k + 1)

        return carry

    lax.fori_loop(0, blocks, backward_block, 0)
    own_d.start()
    relay_block(0)

    def settle(j, carry):
        source = lax.rem(me + dp_total - j, dp_total)
        for copy in (hand_x(j, source), hand_h(j, source)):
            copy.wait_send()
            copy.wait_recv()
        return carry

    lax.fori_loop(1, dp_total, settle, 0)
    whole = pl.ds(0, frames)

    def settle_dpre(j, carry):
        spread(j, 0, whole, me).wait_send()
        relay(j, whole, source_of(me, j)).wait_send()
        relay(j, whole, source_of(partner, j)).wait_recv()
        return carry

    lax.fori_loop(1, dp_total // 2, settle_dpre, 0)
    to_partner(whole, me).wait_send()
    to_partner(whole, partner).wait_recv()

    def drain(k, carry):
        @pl.when(stage < pipe_total - 1)
        def _():
            up(k).wait_send()

        @pl.when(stage > 0)
        def _():
            down(k).wait_send()

        return carry

    lax.fori_loop(0, blocks, drain, 0)
    own_x.wait()
    own_h.wait()
    own_d.wait()


def contract_rows(left, right):
    return lax.dot_general(
        left, right, (((0,), (0,)), ((), ())), preferred_element_type=F32
    )


def local(inputs, input_weight, recurrent_weight, gate_bias, lengths, cotangent):
    frames, utterances, width = inputs.shape
    gate_width = 4 * width
    dp_total = lax.axis_size("dp")
    pipe_total = lax.axis_size("pipe")
    me = lax.axis_index("dp")
    own_width = width // dp_total
    share = max(own_width, 128)
    blocks = frames // SPAN
    live = (jnp.arange(frames, dtype=jnp.int32)[:, None] < lengths[None, :]).astype(F32)
    live = jnp.broadcast_to(live[:, :, None], (frames, utterances, 128))
    vmem = pl.BlockSpec(memory_space=pltpu.VMEM)
    hbm = pl.BlockSpec(memory_space=pl.ANY)
    dma = pltpu.SemaphoreType.DMA
    dpre_all, x_all, h_all, hidden, cell = pl.pallas_call(
        partial(kernel, dp_total, pipe_total, own_width, share),
        out_shape=(
            jax.ShapeDtypeStruct((dp_total, frames, utterances, gate_width), BF16),
            jax.ShapeDtypeStruct((dp_total, frames, utterances, share), BF16),
            jax.ShapeDtypeStruct((dp_total, frames, utterances, share), BF16),
            jax.ShapeDtypeStruct((utterances, width), BF16),
            jax.ShapeDtypeStruct((utterances, width), F32),
        ),
        in_specs=[hbm, hbm, hbm, vmem, vmem, vmem],
        out_specs=(hbm, hbm, hbm, vmem, vmem),
        scratch_shapes=[
            pltpu.VMEM((width, gate_width), BF16),
            pltpu.VMEM((width, gate_width), BF16),
            pltpu.VMEM((gate_width, width), BF16),
            pltpu.VMEM((gate_width, width), BF16),
            pltpu.VMEM((frames, utterances, width), BF16),
            pltpu.VMEM((frames, utterances, width), BF16),
            pltpu.VMEM((frames + 1, utterances, width), BF16),
            pltpu.VMEM((frames + 1, utterances, width), F32),
            pltpu.VMEM((frames, utterances, gate_width), F32),
            pltpu.VMEM((SPAN, utterances, gate_width), F32),
            pltpu.VMEM((frames, utterances, gate_width), BF16),
            pltpu.VMEM((frames, utterances, width), BF16),
            pltpu.VMEM((frames, utterances, width), BF16),
            pltpu.VMEM((utterances, width), F32),
            pltpu.VMEM((utterances, width), F32),
            dma((3,)),
            dma((blocks,)),
            dma((blocks,)),
            dma((blocks,)),
            dma((blocks,)),
            dma((1,)),
            dma((1,)),
            dma((dp_total // 2 - 1,)),
            dma(((dp_total // 2 - 1) * blocks,)),
            dma((dp_total // 2 - 1,)),
            dma((dp_total // 2 - 1,)),
            dma((dp_total - 1,)),
            dma((dp_total - 1,)),
            dma((dp_total - 1,)),
            dma((dp_total - 1,)),
            dma((3,)),
        ],
        compiler_params=pltpu.CompilerParams(
            collective_id=0, has_side_effects=True, vmem_limit_bytes=52 * 1024 * 1024
        ),
    )(inputs, input_weight[0], recurrent_weight[0], gate_bias, live, cotangent[0])
    if share > own_width:
        offset = (me * own_width) % share
        x_all = lax.dynamic_slice_in_dim(x_all, offset, own_width, 3)
        h_all = lax.dynamic_slice_in_dim(h_all, offset, own_width, 3)
    rows = dpre_all.reshape(-1, gate_width)
    input_grad = contract_rows(x_all.reshape(-1, own_width), rows)
    recurrent_grad = contract_rows(h_all.reshape(-1, own_width), rows)
    bias_width = gate_width // dp_total
    mine = lax.dynamic_slice_in_dim(rows, me * bias_width, bias_width, 1)
    bias_grad = jnp.sum(mine.astype(F32), axis=0)
    return (input_grad[None], recurrent_grad[None], bias_grad[None], hidden[None], cell[None])


def solution(mesh):
    return jax.shard_map(
        local,
        mesh=mesh,
        in_specs=(
            P(None, "dp", None),
            P("pipe", None, None),
            P("pipe", None, None),
            P("pipe", None),
            P("dp"),
            P("pipe", None, "dp", None),
        ),
        out_specs=(
            P("pipe", "dp", None),
            P("pipe", "dp", None),
            P("pipe", "dp"),
            P("pipe", "dp", None),
            P("pipe", "dp", None),
        ),
        check_vma=False,
    )
```
